16 devices in a mesh: stage: 2 (over z), expert: 8 (over y, x, core).
Axes of the slice: x: 2, y: 2, z: 2, core: 2. Of those that a mesh axis runs over, the one named last changes fastest.
Arguments:
- w_gate: bfloat16 [4, 8, 2048, 1024], P('stage', 'expert')
- w_up: bfloat16 [4, 8, 2048, 1024], P('stage', 'expert')
- w_down: bfloat16 [4, 8, 1024, 2048], P('stage', 'expert')
- dense: bfloat16 [4, 2048, 2048], P('stage')
- hot_ids: int32 [2], replicated
- spare_map: int32 [16], P(('stage', 'expert'))
Outputs:
- output 1: bfloat16 [4, 16, 2048, 1024], P(None, ('stage', 'expert'))
- output 2: bfloat16 [4, 16, 512, 2048], P(None, ('stage', 'expert'))
- output 3: bfloat16 [4, 2048, 2048], replicated
- output 4: bfloat16 [4, 16, 2048, 1024], P(None, ('stage', 'expert'))
- output 5: bfloat16 [4, 16, 512, 2048], P(None, ('stage', 'expert'))
All inputs are finite; a program needn't handle non-finite values.
Results may differ from the reference program's by a relative error of at most 0.001.
Values are sent between devices in bfloat16 or wider.
A program may use at most 1 GiB of HBM per device.

```python
import jax
import jax.numpy as jnp

LAYERS = 4
EXPERTS = 8
D_MODEL = 2048
FF_WIDTH = 1024
DENSE_WIDTH = 2048
PIECES = 2
STAGES = 2
GROUPS = 8
DEVICES = 16
HOT_UNITS = 2

PIECE_WIDTH = FF_WIDTH // PIECES
UNIT_COUNT = EXPERTS * PIECES
PER_DEVICE = UNIT_COUNT // DEVICES


def draw_placement(base_key):
    key_list = jax.random.split(base_key, 6)
    first_dev = jax.random.randint(key_list[0], (), 0, DEVICES, dtype=jnp.int32)
    shift_stage = jax.random.randint(key_list[1], (), 1, STAGES, dtype=jnp.int32)
    shift_group = jax.random.randint(key_list[2], (), 1, GROUPS, dtype=jnp.int32)
    second_stage = (first_dev // GROUPS + shift_stage) % STAGES
    second_group = (first_dev % GROUPS + shift_group) % GROUPS
    second_dev = second_stage * GROUPS + second_group
    offsets = jax.random.randint(key_list[3], (HOT_UNITS,), 0, PER_DEVICE, dtype=jnp.int32)
    hot_ids = jnp.stack([first_dev, second_dev]) * PER_DEVICE + offsets
    base_map = jax.random.randint(key_list[4], (DEVICES,), -1, HOT_UNITS, dtype=jnp.int32)
    slot_order = jax.random.permutation(key_list[5], DEVICES)
    forced = jnp.concatenate([jnp.arange(HOT_UNITS, dtype=jnp.int32), jnp.full((1,), -1, dtype=jnp.int32)])
    spare_map = base_map.at[slot_order[:HOT_UNITS + 1]].set(forced)
    return hot_ids.astype(jnp.int32), spare_map.astype(jnp.int32)


def setup_inputs(seed: int = 0) -> dict:
    key_list = jax.random.split(jax.random.key(seed), 5)
    expert_shape = (LAYERS, EXPERTS, D_MODEL, FF_WIDTH)
    w_gate = jax.random.normal(key_list[0], expert_shape, jnp.float32).astype(jnp.bfloat16)
    w_up = jax.random.normal(key_list[1], expert_shape, jnp.float32).astype(jnp.bfloat16)
    w_down = jax.random.normal(key_list[2], (LAYERS, EXPERTS, FF_WIDTH, D_MODEL), jnp.float32).astype(jnp.bfloat16)
    dense = jax.random.normal(key_list[3], (LAYERS, D_MODEL, DENSE_WIDTH), jnp.float32).astype(jnp.bfloat16)
    hot_ids, spare_map = draw_placement(key_list[4])
    return {'w_gate': w_gate, 'w_up': w_up, 'w_down': w_down, 'dense': dense, 'hot_ids': hot_ids, 'spare_map': spare_map}


def reference(w_gate, w_up, w_down, dense, hot_ids, spare_map):
    gate_parts = w_gate.reshape(LAYERS, EXPERTS, D_MODEL, PIECES, PIECE_WIDTH)
    up_parts = w_up.reshape(LAYERS, EXPERTS, D_MODEL, PIECES, PIECE_WIDTH)
    gate_up = jnp.concatenate([gate_parts, up_parts], axis=-1)
    gate_up = jnp.transpose(gate_up, (0, 1, 3, 2, 4)).reshape(LAYERS, UNIT_COUNT, D_MODEL, 2 * PIECE_WIDTH)
    down_units = w_down.reshape(LAYERS, UNIT_COUNT, PIECE_WIDTH, D_MODEL)
    hot_gate_up = jnp.take(gate_up, hot_ids, axis=1)
    hot_down = jnp.take(down_units, hot_ids, axis=1)
    slot_index = jnp.maximum(spare_map, 0)
    filled = (spare_map >= 0)[None, :, None, None]
    spare_gate_up = jnp.where(filled, jnp.take(hot_gate_up, slot_index, axis=1), jnp.zeros((), gate_up.dtype))
    spare_down = jnp.where(filled, jnp.take(hot_down, slot_index, axis=1), jnp.zeros((), down_units.dtype))
    return gate_up, down_units, dense, spare_gate_up, spare_down
```

```python
import jax
import jax.numpy as jnp
from jax import lax
from jax.experimental import pallas as pl
from jax.experimental.pallas import tpu as pltpu
from jax.sharding import PartitionSpec as P

MESH = pl.DeviceIdType.MESH
ANY = pl.BlockSpec(memory_space=pl.ANY)
BF16 = jnp.bfloat16
DIRECT = 256
QUARTER = (2048 - DIRECT) // 4
HALF = QUARTER // 2
CHUNKS = 32


def coords():
    s = lax.axis_index('stage')
    g = lax.axis_index('expert')
    return s, g // 4, (g // 2) % 2, g % 2


def dev(z, y, x, c):
    return (z, y * 4 + x * 2 + c)


def remote(src, dst, send_sem, recv_sem, target):
    return pltpu.make_async_remote_copy(
        src_ref=src, dst_ref=dst, send_sem=send_sem, recv_sem=recv_sem,
        device_id=dev(*target), device_id_type=MESH)


def move_kernel(gate, up, down, dense, w13, w2, other, us, ur, ul, ds, dr):
    z, y, x, c = coords()
    is_s = c == x
    is_r = c != x

    def quarter(yy, xx):
        return pl.multiple_of(DIRECT + (yy * 2 + xx) * QUARTER, 32)

    q0 = quarter(y, x)
    zn = (1 - z, y, x, c)
    sib = (z, y, x, 1 - c)
    xn = (z, y, 1 - x, c)
    yn = (z, 1 - y, x, c)
    zq = remote(dense.at[c, pl.ds(q0, QUARTER)], other.at[c, pl.ds(q0, QUARTER)], ds.at[0], dr.at[0], zn)
    zd = remote(dense.at[c, pl.ds(0, DIRECT)], other.at[c, pl.ds(0, DIRECT)], ds.at[1], dr.at[1], zn)
    zq.start()
    zd.start()

    unit_copies = []
    for p in range(2):
        same = (y == z) & (x == y) & (c == x) & (p == c)
        dst_chip = (y, x, c, p)
        triples = [
            (gate.at[:, 0, :, pl.ds(p * 512, 512)], w13.at[pl.ds(2 * z, 2), 0, :, pl.ds(0, 512)]),
            (up.at[:, 0, :, pl.ds(p * 512, 512)], w13.at[pl.ds(2 * z, 2), 0, :, pl.ds(512, 512)]),
            (down.at[:, 0, pl.ds(p * 512, 512), :], w2.at[pl.ds(2 * z, 2), 0]),
        ]
        for k, (src, dst) in enumerate(triples):
            cp = remote(src, dst, us.at[p, k], ur.at[z, k], dst_chip)
            lc = pltpu.make_async_copy(src, dst, ul.at[k])
            unit_copies.append((same, cp, lc))
    for same, cp, lc in unit_copies:
        @pl.when(jnp.logical_not(same))
        def _():
            cp.start()

        @pl.when(same)
        def _():
            lc.start()

    def band(ref, start, size, layer=None):
        if layer is None:
            return ref.at[:, pl.ds(start, size)]
        return ref.at[layer, pl.ds(start, size)]

    zq.wait_recv()
    dq = remote(band(other, q0, QUARTER, c), band(other, q0, QUARTER, c), ds.at[2], dr.at[2], sib)
    dq.start()
    zd.wait_recv()
    dd = remote(band(other, 0, DIRECT, c), band(other, 0, DIRECT, c), ds.at[3], dr.at[3], sib)
    dd.start()
    dq.wait_recv()

    qx, qy, qd = quarter(y, 1 - x), quarter(1 - y, x), quarter(1 - y, 1 - x)
    xq = remote(band(other, q0, QUARTER), band(other, q0, QUARTER), ds.at[4], dr.at[4], xn)
    yq = remote(band(other, q0, QUARTER), band(other, q0, QUARTER), ds.at[5], dr.at[5], yn)
    ya = remote(band(other, qx, HALF), band(other, qx, HALF), ds.at[6], dr.at[6], yn)
    b0 = pl.multiple_of(qy + HALF, 32)
    xb = remote(band(other, b0, HALF), band(other, b0, HALF), ds.at[7], dr.at[7], xn)
    dx = remote(band(other, qx, QUARTER), band(other, qx, QUARTER), ds.at[8], dr.at[8], sib)
    dy = remote(band(other, qy, QUARTER), band(other, qy, QUARTER), ds.at[9], dr.at[9], sib)
    da = remote(band(other, qd, HALF), band(other, qd, HALF), ds.at[10], dr.at[10], sib)
    e0 = pl.multiple_of(qd + HALF, 32)
    db = remote(band(other, e0, HALF), band(other, e0, HALF), ds.at[11], dr.at[11], sib)

    @pl.when(is_s)
    def _():
        xq.start()
        dy.wait_recv()
        xb.start()
        dx.wait_recv()
        da.wait_recv()
        db.wait_recv()
        xq.wait_send()
        xb.wait_send()

    @pl.when(is_r)
    def _():
        yq.start()
        yq.wait_recv()
        dy.start()
        xq.wait_recv()
        ya.start()
        dx.start()
        ya.wait_recv()
        da.start()
        xb.wait_recv()
        db.start()
        for cp in (yq, ya, dx, dy, da, db):
            cp.wait_send()

    for cp in (zq, zd, dq, dd):
        cp.wait_send()
    dd.wait_recv()

    for zz in range(2):
        same = (zz == z) & (z == y) & (y == x) & (x == c)
        for k, dst in enumerate([w13.at[pl.ds(2 * zz, 2), 0, :, pl.ds(0, 512)],
                                 w13.at[pl.ds(2 * zz, 2), 0, :, pl.ds(512, 512)],
                                 w2.at[pl.ds(2 * zz, 2), 0]]):
            @pl.when(jnp.logical_not(same))
            def _():
                pltpu.make_async_copy(dst, dst, ur.at[zz, k]).wait()
    for same, cp, lc in unit_copies:
        @pl.when(jnp.logical_not(same))
        def _():
            cp.wait_send()

        @pl.when(same)
        def _():
            lc.wait()


def tree_slices(k):
    rows13 = 4096 // CHUNKS
    rows2 = 2048 // CHUNKS
    per13 = 2048 // rows13
    per2 = 512 // rows2
    return [
        (0, (k // per13, 0, pl.ds(pl.multiple_of((k % per13) * rows13, rows13), rows13))),
        (0, (2 + k // per13, 0, pl.ds(pl.multiple_of((k % per13) * rows13, rows13), rows13))),
        (1, (k // per2, 0, pl.ds(pl.multiple_of((k % per2) * rows2, rows2), rows2))),
    ]


def tree_wholes(arrays):
    return [arrays[0].at[pl.ds(0, 2)], arrays[0].at[pl.ds(2, 2)], arrays[1]]


def spread_kernel(root, w13, w2, hot13, hot2, recv, send, csend, crecv):
    rz, ry, rx, rc = root // 8, (root // 4) % 2, (root // 2) % 2, root % 2
    z, y, x, c = coords()
    rel = [x if rx == 0 else 1 - x, y if ry == 0 else 1 - y, z if rz == 0 else 1 - z]
    near = [(z, y, 1 - x, c), (z, 1 - y, x, c), (1 - z, y, x, c)]
    sib = (z, y, x, 1 - c)
    mine = (w13, w2)
    hot = (hot13, hot2)
    relay = c == rc
    at_root = (rel[0] + rel[1] + rel[2]) == 0
    plans = []
    for j in range(3):
        ra, rb, rd = rel[j], rel[(j + 1) % 3], rel[(j + 2) % 3]
        depth = jnp.where(ra == 1, 1 + rb + rd, jnp.where(rb + rd == 0, 0, 2 + rb + rd))
        goes = [
            ((ra + rb + rd) == 0) | ((ra == 1) & ((rb + rd) > 0)),
            (ra == 1) & (rb == 0) & (rd == 0),
            (ra == 1) & (rd == 0),
        ]
        plans.append((depth, goes))

    @pl.when(relay)
    def _():
        def issue(source, j, k, which, index):
            depth, goes = plans[j]
            for step in range(3):
                cp = remote(source[which].at[index], hot[which].at[index],
                            send.at[j, step], recv.at[j, k], near[(j + step) % 3])

                @pl.when(goes[step])
                def _():
                    cp.start()
            remote(source[which].at[index], hot[which].at[index], csend.at[j], crecv.at[j], sib).start()

        @pl.when(at_root)
        def _():
            @pl.loop(0, CHUNKS)
            def _(k):
                for j, (which, index) in enumerate(tree_slices(k)):
                    depth, goes = plans[j]
                    cp = remote(mine[which].at[index], hot[which].at[index],
                                send.at[j, 0], recv.at[j, k], near[j])
                    cp.start()
                for j, (which, index) in enumerate(tree_slices(k)):
                    remote(mine[which].at[index], hot[which].at[index], csend.at[j], crecv.at[j], sib).start()

        @pl.when(jnp.logical_not(at_root))
        def _():
            @pl.loop(1, CHUNKS + 4)
            def _(i):
                for j in range(3):
                    depth, goes = plans[j]
                    k = i - depth

                    @pl.when((k >= 0) & (k < CHUNKS))
                    def _():
                        which, index = tree_slices(k)[j]
                        here = hot[which].at[index]
                        pltpu.make_async_copy(here, here, recv.at[j, k]).wait()
                        issue(hot, j, k, which, index)

        for j, whole in enumerate(tree_wholes(hot)):
            depth, goes = plans[j]
            for step in range(3):
                @pl.when(goes[step])
                def _():
                    pltpu.make_async_copy(whole, whole, send.at[j, step]).wait()
            pltpu.make_async_copy(whole, whole, csend.at[j]).wait()

    @pl.when(jnp.logical_not(relay))
    def _():
        for j, whole in enumerate(tree_wholes(hot)):
            pltpu.make_async_copy(whole, whole, crecv.at[j]).wait()


def pick_kernel(pick, a13, b13, c13, a2, b2, c2, out13, out2):
    for k, (r13, r2) in enumerate(((a13, a2), (b13, b2), (c13, c2))):
        @pl.when(pick[0] == k)
        def _():
            out13[...] = r13[...]
            out2[...] = r2[...]

    @pl.when(pick[0] == 3)
    def _():
        out13[...] = jnp.zeros_like(out13)
        out2[...] = jnp.zeros_like(out2)


def join_kernel(stage, own, other, out):
    layer = pl.program_id(0)

    @pl.when(layer // 2 == stage[0])
    def _():
        out[...] = own[...]

    @pl.when(layer // 2 != stage[0])
    def _():
        out[...] = other[...]


def solution(mesh):
    flat_axes = ('stage', 'expert')
    DMA = pltpu.SemaphoreType.DMA
    side = pltpu.CompilerParams(has_side_effects=True)

    def local_move(w_gate, w_up, w_down, dense, hot_ids, spare_map):
        u13 = jax.ShapeDtypeStruct((4, 1, 2048, 1024), BF16)
        u2 = jax.ShapeDtypeStruct((4, 1, 512, 2048), BF16)
        w13, w2, other = pl.pallas_call(
            move_kernel,
            out_shape=(u13, u2, jax.ShapeDtypeStruct((2, 2048, 2048), BF16)),
            in_specs=[ANY] * 4,
            out_specs=(ANY, ANY, ANY),
            scratch_shapes=[DMA((2, 3)), DMA((2, 3)), DMA((3,)), DMA((12,)), DMA((12,))],
            compiler_params=side,
            name='move',
        )(w_gate, w_up, w_down, dense)

        def spread(root):
            def call(a, b):
                return pl.pallas_call(
                    lambda *refs: spread_kernel(root, *refs),
                    out_shape=(u13, u2),
                    in_specs=[ANY] * 2,
                    out_specs=(ANY, ANY),
                    scratch_shapes=[DMA((3, CHUNKS)), DMA((3, 3)), DMA((3,)), DMA((3,))],
                    compiler_params=side,
                    name='spread%d' % root,
                )(a, b)
            return call

        branches = [spread(root) for root in range(16)]
        a13, a2 = lax.switch(hot_ids[0], branches, w13, w2)
        b13, b2 = lax.switch(hot_ids[1], branches, w13, w2)

        stage = lax.axis_index('stage').astype(jnp.int32)
        rows = 1024
        dense_all = pl.pallas_call(
            join_kernel,
            grid_spec=pltpu.PrefetchScalarGridSpec(
                num_scalar_prefetch=1,
                grid=(4, 2048 // rows),
                in_specs=[
                    pl.BlockSpec((1, rows, 2048), lambda l, i, s: (jnp.where(l // 2 == s[0], l % 2, 1 - s[0]), jnp.where(l // 2 == s[0], i, (1 - s[0]) * (2048 // rows - 1)), 0)),
                    pl.BlockSpec((1, rows, 2048), lambda l, i, s: (jnp.where(l // 2 != s[0], l % 2, s[0]), jnp.where(l // 2 != s[0], i, s[0] * (2048 // rows - 1)), 0)),
                ],
                out_specs=pl.BlockSpec((1, rows, 2048), lambda l, i, s: (l, i, 0)),
            ),
            out_shape=jax.ShapeDtypeStruct((4, 2048, 2048), BF16),
            name='join',
        )(stage.reshape(1), dense, other)

        me = stage * 8 + lax.axis_index('expert').astype(jnp.int32)
        want = spare_map[0]
        home = jnp.where(want == 0, hot_ids[0], hot_ids[1])
        pick = jnp.where(want < 0, 3, jnp.where(home == me, 2, want)).astype(jnp.int32)

        def spec(shape, source):
            def index(l, i, s):
                on = s[0] == source
                return (jnp.where(on, l, 0), 0, jnp.where(on, i, 0), 0)
            return pl.BlockSpec(shape, index)

        s13, s2 = (1, 1, 1024, 1024), (1, 1, 256, 2048)
        spare13, spare2 = pl.pallas_call(
            pick_kernel,
            grid_spec=pltpu.PrefetchScalarGridSpec(
                num_scalar_prefetch=1,
                grid=(4, 2),
                in_specs=[spec(s13, k) for k in range(3)] + [spec(s2, k) for k in range(3)],
                out_specs=[pl.BlockSpec(s13, lambda l, i, s: (l, 0, i, 0)),
                           pl.BlockSpec(s2, lambda l, i, s: (l, 0, i, 0))],
            ),
            out_shape=(u13, u2),
            name='pick',
        )(pick.reshape(1), a13, b13, w13, a2, b2, w2)
        return w13, w2, dense_all, spare13, spare2

    expert_spec = P('stage', 'expert', None, None)
    unit_spec = P(None, flat_axes, None, None)
    return jax.shard_map(
        local_move,
        mesh=mesh,
        in_specs=(expert_spec, expert_spec, expert_spec, P('stage', None, None), P(None), P(flat_axes)),
        out_specs=(unit_spec, unit_spec, P(None, None, None), unit_spec, unit_spec),
        check_vma=False,
    )
```

```python
import jax
import jax.numpy as jnp
from jax import lax
from jax.experimental import pallas as pl
from jax.experimental.pallas import tpu as pltpu
from jax.sharding import PartitionSpec as P


MESH = pl.DeviceIdType.MESH
ANY = pl.BlockSpec(memory_space=pl.ANY)
BF16 = jnp.bfloat16
CHUNKS = 16
SLACK = 3
ROWS = 32
DIRECT = 8
QUARTER = 14


def coords():
    s = lax.axis_index('stage')
    g = lax.axis_index('expert')
    return s, g // 4, (g // 2) % 2, g % 2


def remote(src, dst, send_sem, recv_sem, target):
    z, y, x, c = target
    return pltpu.make_async_remote_copy(
        src_ref=src, dst_ref=dst, send_sem=send_sem, recv_sem=recv_sem,
        device_id=(z, y * 4 + x * 2 + c), device_id_type=MESH)


def arrived(ref, sem):
    pltpu.make_async_copy(ref, ref, sem).wait()


def spread_kernel(unit, layer, gate, up, down, dense, hot13, hot2, other,
                  recv, send, qrecv, trecv, qsend):
    expert, piece = unit // 2, unit % 2
    ry, rx, rc = expert // 4, (expert // 2) % 2, expert % 2
    z, y, x, c = coords()
    is_r = c != x
    is_s = c == x
    late = jnp.where(is_s, 1, 0)
    near = [(z, y, 1 - x, c), (z, 1 - y, x, c), (1 - z, y, x, c), (z, y, x, 1 - c)]
    rel_x = x if rx == 0 else 1 - x
    rel_y = y if ry == 0 else 1 - y

    def tree(t):
        h, j = t // 3, t % 3
        rel = [rel_x, rel_y, (z + h) % 2]
        pick = lambda n: jnp.where(n == 0, rel[0], jnp.where(n == 1, rel[1], rel[2]))
        ra, rd = pick(j), pick((j + 2) % 3)
        total = rel[0] + rel[1] + rel[2]
        at_root = total == 0
        origin = at_root & (c == rc)
        first = at_root | ((ra == 1) & (total > 1))
        second = (ra == 1) & (total == 1)
        third = (ra == 1) & (rd == 0)
        goes = []
        for d, who in enumerate((is_s, is_r, is_r)):
            turn = (d + 3 - j) % 3
            goes.append(who & (((turn == 0) & first) | ((turn == 1) & second) | ((turn == 2) & third)))
        goes.append(is_r | at_root)
        depth = jnp.where(ra == 1, total, 2 + total)
        lag = jnp.where(at_root, jnp.where(origin, 0, 1), SLACK * depth + late)
        return h, j, goes, origin, lag

    def hot13_at(h, j, k):
        rows = 4096 // CHUNKS
        l, r = k // (CHUNKS // 2), k % (CHUNKS // 2)
        band = pl.ds(pl.multiple_of(r * rows, rows), rows)
        here = hot13.at[2 * h + l, 0, band, pl.ds(pl.multiple_of(j * 512, 512), 512)]
        return here, (l, 0, band, pl.ds(piece * 512, 512))

    def hot2_at(h, k):
        rows = 1024 // CHUNKS
        l, r = k // (CHUNKS // 2), k % (CHUNKS // 2)
        here = hot2.at[2 * h + l, 0, pl.ds(pl.multiple_of(r * rows, rows), rows), :]
        return here, (l, 0, pl.ds(pl.multiple_of(piece * 512 + r * rows, rows), rows), slice(None))

    def rows_of(s, m):
        q = ((y + s // 2) % 2) * 2 + (x + s % 2) % 2
        return pl.ds(pl.multiple_of((DIRECT + q * QUARTER + m) * ROWS, ROWS), ROWS)

    @pl.loop(0, CHUNKS + 4 * SLACK + 2)
    def _(i):
        @pl.when(is_r & (i < QUARTER))
        def _():
            rows = rows_of(0, i)
            remote(dense.at[layer, rows], other.at[rows], qsend.at[0], qrecv.at[0, i], near[2]).start()

        @pl.when(is_r & (i < DIRECT))
        def _():
            rows = pl.ds(pl.multiple_of(i * ROWS, ROWS), ROWS)
            remote(dense.at[layer, rows], other.at[rows], qsend.at[1], trecv.at[i], near[2]).start()

        @pl.loop(0, 6)
        def _(t):
            h, j, goes, origin, lag = tree(t)
            k = i - lag

            def pass_on(source, here):
                for d in range(4):
                    @pl.when(goes[d])
                    def _():
                        remote(source, here, send.at[t, d], recv.at[t, k], near[d]).start()

            def give(source, here):
                @pl.loop(0, 4)
                def _(d):
                    on = (goes[0] & (d == 0)) | (goes[1] & (d == 1)) | (goes[2] & (d == 2)) | (goes[3] & (d == 3))

                    @pl.when(on)
                    def _():
                        flip = lambda bit, n: jnp.where(d == n, 1 - bit, bit)
                        remote(source, here, send.at[t, d], recv.at[t, k],
                               (flip(z, 2), flip(y, 1), flip(x, 0), flip(c, 3))).start()

            @pl.when((k >= 0) & (k < CHUNKS))
            def _():
                @pl.when(j < 2)
                def _():
                    here, index = hot13_at(h, j, k)
                    for n, source in enumerate((gate, up)):
                        @pl.when(origin & (j == n))
                        def _():
                            give(source.at[index], here)

                    @pl.when(jnp.logical_not(origin))
                    def _():
                        arrived(here, recv.at[t, k])
                        pass_on(here, here)

                @pl.when(j == 2)
                def _():
                    here, index = hot2_at(h, k)

                    @pl.when(origin)
                    def _():
                        give(down.at[index], here)

                    @pl.when(jnp.logical_not(origin))
                    def _():
                        arrived(here, recv.at[t, k])
                        pass_on(here, here)

        @pl.loop(0, 4)
        def _(s):
            m = i - (SLACK + (SLACK + 1) * (s % 2) + SLACK * (s // 2) + late)

            @pl.when((m >= 0) & (m < QUARTER))
            def _():
                rows = rows_of(s, m)
                here = other.at[rows]
                arrived(here, qrecv.at[s, m])

                @pl.when(is_r & ((s == 0) | ((s == 1) & (m % 2 == 0))))
                def _():
                    remote(here, here, qsend.at[2], qrecv.at[s + 2, m], near[1]).start()

                @pl.when(is_s & ((s == 0) | ((s == 2) & (m % 2 == 1))))
                def _():
                    remote(here, here, qsend.at[3], qrecv.at[s + 1, m], near[0]).start()

                @pl.when(is_r)
                def _():
                    remote(here, here, qsend.at[4], qrecv.at[s, m], near[3]).start()

        m = i - (SLACK + late)

        @pl.when((m >= 0) & (m < DIRECT))
        def _():
            here = other.at[pl.ds(pl.multiple_of(m * ROWS, ROWS), ROWS)]
            arrived(here, trecv.at[m])

            @pl.when(is_r)
            def _():
                remote(here, here, qsend.at[5], trecv.at[m], near[3]).start()

    @pl.loop(0, 6)
    def _(t):
        _, _, goes, origin, _ = tree(t)

        @pl.when(origin)
        def _():
            @pl.loop(0, CHUNKS)
            def _(k):
                arrived(hot2_at(0, 0)[0], recv.at[t, k])

        for d in range(4):
            @pl.when(goes[d])
            def _():
                arrived(hot2.at[pl.ds(0, 2)], send.at[t, d])

    quarter, direct = QUARTER * ROWS, DIRECT * ROWS

    @pl.when(is_r)
    def _():
        arrived(other.at[pl.ds(0, quarter)], qsend.at[0])
        arrived(other.at[pl.ds(0, direct)], qsend.at[1])
        arrived(other.at[pl.ds(0, quarter + quarter // 2)], qsend.at[2])
        arrived(other.at[pl.ds(0, 4 * quarter)], qsend.at[4])
        arrived(other.at[pl.ds(0, direct)], qsend.at[5])

    @pl.when(is_s)
    def _():
        arrived(other.at[pl.ds(0, quarter + quarter // 2)], qsend.at[3])


def cut_kernel(stage, gate, up, a13, b13):
    for s, (left, right) in enumerate(((a13, b13), (b13, a13))):
        @pl.when(stage[0] == s)
        def _():
            left[0, :, :512] = gate[0, 0, :, :512]
            left[0, :, 512:] = up[0, 0, :, :512]
            right[0, :, :512] = gate[0, 0, :, 512:]
            right[0, :, 512:] = up[0, 0, :, 512:]


def copy_kernel(pick, *refs):
    *sources, out = refs
    choice = pick[pl.program_id(0)]
    for k, ref in enumerate(sources):
        @pl.when(choice == k)
        def _():
            out[...] = ref[...].reshape(out.shape)

    @pl.when(choice == len(sources))
    def _():
        out[...] = jnp.zeros_like(out)


def pick_layers(picks, where, to, sources, shape, rows, base=None):
    blocks = shape[-2] // rows
    count = picks.shape[0]
    table = jnp.concatenate([picks, where, to]).astype(jnp.int32)

    def spec(k, source):
        lead = (1,) * (len(source.shape) - 2)

        def index(n, i, t):
            on = t[n] == k
            return (jnp.where(on, t[count + n], 0),) + (0,) * (len(lead) - 1) + (jnp.where(on, i, 0), 0)

        return pl.BlockSpec(lead + (rows, shape[-1]), index)

    lead = (1,) * (len(shape) - 2)
    extra = [] if base is None else [base]
    body = copy_kernel if base is None else lambda pick, kept, *refs: copy_kernel(pick, *refs)
    return pl.pallas_call(
        body,
        grid_spec=pltpu.PrefetchScalarGridSpec(
            num_scalar_prefetch=1,
            grid=(count, blocks),
            in_specs=[ANY] * len(extra) + [spec(k, source) for k, source in enumerate(sources)],
            out_specs=pl.BlockSpec(
                lead + (rows, shape[-1]), lambda n, i, t: (t[2 * count + n],) + (0,) * (len(lead) - 1) + (i, 0)),
        ),
        out_shape=jax.ShapeDtypeStruct(shape, BF16),
        input_output_aliases={} if base is None else {1: 0},
        cost_estimate=pl.CostEstimate(flops=0, bytes_accessed=4 * count * shape[-2] * shape[-1], transcendentals=0),
    )(table, *extra, *sources)


def permute_pairs(swap):
    pairs = [(z * 8 + e, 2 * e + (1 - z if swap else z)) for z in range(2) for e in range(8)]
    return [(a, b) for a, b in pairs if a != b]


def solution(mesh):
    flat_axes = ('stage', 'expert')
    DMA = pltpu.SemaphoreType.DMA
    side = pltpu.CompilerParams(has_side_effects=True)
    u13 = jax.ShapeDtypeStruct((4, 1, 2048, 1024), BF16)
    u2 = jax.ShapeDtypeStruct((4, 1, 512, 2048), BF16)

    def spread(unit, layer):
        def call(*args):
            return pl.pallas_call(
                lambda *refs: spread_kernel(unit, layer, *refs),
                out_shape=(u13, u2, jax.ShapeDtypeStruct((2048, 2048), BF16)),
                in_specs=[ANY] * 4,
                out_specs=(ANY, ANY, ANY),
                scratch_shapes=[DMA((6, CHUNKS)), DMA((6, 4)), DMA((4, QUARTER)), DMA((DIRECT,)), DMA((6,))],
                compiler_params=side,
                cost_estimate=pl.CostEstimate(flops=0, bytes_accessed=300 << 20, transcendentals=0),
            )(*args)

        return call

    def local_move(w_gate, w_up, w_down, dense, hot_ids, spare_map):
        stage = lax.axis_index('stage').astype(jnp.int32)
        core = (lax.axis_index('expert') % 2).astype(jnp.int32)
        layers = jnp.arange(4, dtype=jnp.int32)

        def permute(value, swap):
            return lax.ppermute(value, flat_axes, permute_pairs(swap))

        def slice2(piece):
            return pl.pallas_call(
                lambda t, ref, out: copy_kernel(t, ref, out),
                grid_spec=pltpu.PrefetchScalarGridSpec(
                    num_scalar_prefetch=1,
                    grid=(2, 2),
                    in_specs=[pl.BlockSpec((1, 1, 256, 2048), lambda l, i, t: (l, 0, 2 * t[2] + i, 0))],
                    out_specs=pl.BlockSpec((1, 256, 2048), lambda l, i, t: (l, i, 0)),
                ),
                out_shape=jax.ShapeDtypeStruct((2, 512, 2048), BF16),
            )(jnp.stack([0 * piece, 0 * piece, piece]), w_down)

        own2 = slice2(stage)
        own2, later = lax.optimization_barrier((own2, stage))
        a2 = permute(own2, 0)
        far2 = slice2(1 - later)
        b2 = permute(far2, 1)
        rows = 512
        own13, far13 = pl.pallas_call(
            cut_kernel,
            grid_spec=pltpu.PrefetchScalarGridSpec(
                num_scalar_prefetch=1,
                grid=(2, 2048 // rows),
                in_specs=[pl.BlockSpec((1, 1, rows, 1024), lambda l, i, s: (l, 0, i, 0))] * 2,
                out_specs=[pl.BlockSpec((1, rows, 1024), lambda l, i, s: (l, i, 0))] * 2,
            ),
            out_shape=(jax.ShapeDtypeStruct((2, 2048, 1024), BF16),) * 2,
            name='cut',
        )(later.reshape(1), w_gate, w_up)

        def spread_all(unit, h):
            branches = [spread(root, h) for root in range(16)]
            return lax.switch(unit, branches, w_gate, w_up, w_down, dense)

        own13, far13, first, second = lax.optimization_barrier((own13, far13, hot_ids[0], hot_ids[1]))
        h13, h2, o0 = spread_all(first, 0)
        own13, o0, second = lax.optimization_barrier((own13, o0, second))
        a13 = permute(own13, 0)
        g13, g2, o1 = spread_all(second, 1)
        far13, o1 = lax.optimization_barrier((far13, o1))
        b13 = permute(far13, 1)

        dense_all = pick_layers(
            jnp.where(layers // 2 == stage, 0, 1 + layers % 2), jnp.where(layers // 2 == stage, layers % 2, 0), layers,
            (dense, o0.reshape(1, 2048, 2048), o1.reshape(1, 2048, 2048)), (4, 2048, 2048), 1024)
        want = jnp.where(spare_map[0] < 0, 2, spare_map[0]) + 0 * layers
        spare13 = pick_layers(want, layers, layers, (h13, g13), u13.shape, 2048)
        spare2 = pick_layers(want, layers, layers, (h2, g2), u2.shape, 512)

        flat = stage * 8 + lax.axis_index('expert').astype(jnp.int32)
        keeps = jnp.where((flat == 0) | (flat == 15), 1, 0)
        pair = layers[:2]
        w2 = pick_layers(jnp.where(layers // 2 == core, keeps, 2), layers % 2, layers, (a2, own2, b2), u2.shape, 512)
        w13 = pick_layers(keeps + 0 * pair, pair, 2 * core + pair, (a13, own13), u13.shape, 2048)
        w13 = pick_layers(0 * pair, pair, 2 - 2 * core + pair, (b13,), u13.shape, 2048, w13)
        return w13, w2, dense_all, spare13, spare2

    expert_spec = P('stage', 'expert', None, None)
    unit_spec = P(None, flat_axes, None, None)

    return jax.shard_map(
        local_move,
        mesh=mesh,
        in_specs=(expert_spec, expert_spec, expert_spec, P('stage', None, None), P(None), P(flat_axes)),
        out_specs=(unit_spec, unit_spec, P(None, None, None), unit_spec, unit_spec),
        check_vma=False,
    )
```

```python
import jax
import jax.numpy as jnp
from jax import lax
from jax.experimental import pallas as pl
from jax.experimental.pallas import tpu as pltpu
from jax.sharding import PartitionSpec as P


MESH = pl.DeviceIdType.MESH
ANY = pl.BlockSpec(memory_space=pl.ANY)
BF16 = jnp.bfloat16
CHUNKS = 16
SLACK = 3
ROWS = 32
DIRECT = 8
QUARTER = 14


def coords():
    s = lax.axis_index('stage')
    g = lax.axis_index('expert')
    return s, g // 4, (g // 2) % 2, g % 2


def remote(src, dst, send_sem, recv_sem, target):
    z, y, x, c = target
    return pltpu.make_async_remote_copy(
        src_ref=src, dst_ref=dst, send_sem=send_sem, recv_sem=recv_sem,
        device_id=(z, y * 4 + x * 2 + c), device_id_type=MESH)


def arrived(ref, sem):
    pltpu.make_async_copy(ref, ref, sem).wait()


def spread_kernel(unit, layer, gate, up, down, dense, hot13, hot2, other, *rest):
    if layer == 0:
        own13, far_a, far_b, recv, send, qrecv, trecv, qsend, local, cut = rest
    else:
        recv, send, qrecv, trecv, qsend = rest
    expert, piece = unit // 2, unit % 2
    ry, rx, rc = expert // 4, (expert // 2) % 2, expert % 2
    z, y, x, c = coords()
    is_r = c != x
    is_s = c == x
    late = jnp.where(is_s, 1, 0)
    near = [(z, y, 1 - x, c), (z, 1 - y, x, c), (1 - z, y, x, c), (z, y, x, 1 - c)]
    rel_x = x if rx == 0 else 1 - x
    rel_y = y if ry == 0 else 1 - y

    def tree(t):
        h, j = t // 3, t % 3
        rel = [rel_x, rel_y, (z + h) % 2]
        pick = lambda n: jnp.where(n == 0, rel[0], jnp.where(n == 1, rel[1], rel[2]))
        ra, rd = pick(j), pick((j + 2) % 3)
        total = rel[0] + rel[1] + rel[2]
        at_root = total == 0
        origin = at_root & (c == rc)
        first = at_root | ((ra == 1) & (total > 1))
        second = (ra == 1) & (total == 1)
        third = (ra == 1) & (rd == 0)
        goes = []
        for d, who in enumerate((is_s, is_r, is_r)):
            turn = (d + 3 - j) % 3
            goes.append(who & (((turn == 0) & first) | ((turn == 1) & second) | ((turn == 2) & third)))
        goes.append(is_r | at_root)
        depth = jnp.where(ra == 1, total, 2 + total)
        lag = jnp.where(at_root, jnp.where(origin, 0, 1), SLACK * depth + late)
        return h, j, goes, origin, lag

    def hot13_at(h, j, k):
        rows = 4096 // CHUNKS
        l, r = k // (CHUNKS // 2), k % (CHUNKS // 2)
        band = pl.ds(pl.multiple_of(r * rows, rows), rows)
        here = hot13.at[2 * h + l, 0, band, pl.ds(pl.multiple_of(j * 512, 512), 512)]
        return here, (l, 0, band, pl.ds(piece * 512, 512))

    def hot2_at(h, k):
        rows = 1024 // CHUNKS
        l, r = k // (CHUNKS // 2), k % (CHUNKS // 2)
        here = hot2.at[2 * h + l, 0, pl.ds(pl.multiple_of(r * rows, rows), rows), :]
        return here, (l, 0, pl.ds(pl.multiple_of(piece * 512 + r * rows, rows), rows), slice(None))

    def rows_of(s, m):
        q = ((y + s // 2) % 2) * 2 + (x + s % 2) % 2
        return pl.ds(pl.multiple_of((DIRECT + q * QUARTER + m) * ROWS, ROWS), ROWS)

    def load(side, n):
        columns = pl.ds(pl.multiple_of(((z + side) % 2) * 512, 512), 512)
        return pltpu.make_async_copy((gate, up)[n].at[:, 0, :, columns], cut.at[side, :, :, pl.ds(n * 512, 512)], local.at[side, n])

    def store(n):
        src = cut.at[0] if n == 0 else cut.at[1, n - 1]
        return pltpu.make_async_copy(src, (own13, far_a, far_b)[n], local.at[2, n])

    if layer == 0:
        for side in range(2):
            for n in range(2):
                load(side, n).start()

    @pl.loop(0, CHUNKS + 4 * SLACK + 2)
    def _(i):
        if layer == 0:
            @pl.when(i == SLACK)
            def _():
                for side in range(2):
                    for n in range(2):
                        load(side, n).wait()
                for n in range(3):
                    store(n).start()

        @pl.when(is_r & (i < QUARTER))
        def _():
            rows = rows_of(0, i)
            remote(dense.at[layer, rows], other.at[rows], qsend.at[0], qrecv.at[0, i], near[2]).start()

        @pl.when(is_r & (i < DIRECT))
        def _():
            rows = pl.ds(pl.multiple_of(i * ROWS, ROWS), ROWS)
            remote(dense.at[layer, rows], other.at[rows], qsend.at[1], trecv.at[i], near[2]).start()

        @pl.loop(0, 6)
        def _(t):
            h, j, goes, origin, lag = tree(t)
            k = i - lag

            def pass_on(source, here):
                for d in range(4):
                    @pl.when(goes[d])
                    def _():
                        remote(source, here, send.at[t, d], recv.at[t, k], near[d]).start()

            def give(source, here):
                @pl.loop(0, 4)
                def _(d):
                    on = (goes[0] & (d == 0)) | (goes[1] & (d == 1)) | (goes[2] & (d == 2)) | (goes[3] & (d == 3))

                    @pl.when(on)
                    def _():
                        flip = lambda bit, n: jnp.where(d == n, 1 - bit, bit)
                        remote(source, here, send.at[t, d], recv.at[t, k],
                               (flip(z, 2), flip(y, 1), flip(x, 0), flip(c, 3))).start()

            @pl.when((k >= 0) & (k < CHUNKS))
            def _():
                @pl.when(j < 2)
                def _():
                    here, index = hot13_at(h, j, k)
                    for n, source in enumerate((gate, up)):
                        @pl.when(origin & (j == n))
                        def _():
                            give(source.at[index], here)

                    @pl.when(jnp.logical_not(origin))
                    def _():
                        arrived(here, recv.at[t, k])
                        pass_on(here, here)

                @pl.when(j == 2)
                def _():
                    here, index = hot2_at(h, k)

                    @pl.when(origin)
                    def _():
                        give(down.at[index], here)

                    @pl.when(jnp.logical_not(origin))
                    def _():
                        arrived(here, recv.at[t, k])
                        pass_on(here, here)

        @pl.loop(0, 4)
        def _(s):
            m = i - (SLACK + (SLACK + 1) * (s % 2) + SLACK * (s // 2) + late)

            @pl.when((m >= 0) & (m < QUARTER))
            def _():
                rows = rows_of(s, m)
                here = other.at[rows]
                arrived(here, qrecv.at[s, m])

                @pl.when(is_r & ((s == 0) | ((s == 1) & (m % 2 == 0))))
                def _():
                    remote(here, here, qsend.at[2], qrecv.at[s + 2, m], near[1]).start()

                @pl.when(is_s & ((s == 0) | ((s == 2) & (m % 2 == 1))))
                def _():
                    remote(here, here, qsend.at[3], qrecv.at[s + 1, m], near[0]).start()

                @pl.when(is_r)
                def _():
                    remote(here, here, qsend.at[4], qrecv.at[s, m], near[3]).start()

        m = i - (SLACK + late)

        @pl.when((m >= 0) & (m < DIRECT))
        def _():
            here = other.at[pl.ds(pl.multiple_of(m * ROWS, ROWS), ROWS)]
            arrived(here, trecv.at[m])

            @pl.when(is_r)
            def _():
                remote(here, here, qsend.at[5], trecv.at[m], near[3]).start()

    @pl.loop(0, 6)
    def _(t):
        _, _, goes, origin, _ = tree(t)

        @pl.when(origin)
        def _():
            @pl.loop(0, CHUNKS)
            def _(k):
                arrived(hot2_at(0, 0)[0], recv.at[t, k])

        for d in range(4):
            @pl.when(goes[d])
            def _():
                arrived(hot2.at[pl.ds(0, 2)], send.at[t, d])

    if layer == 0:
        for n in range(3):
            store(n).wait()

    quarter, direct = QUARTER * ROWS, DIRECT * ROWS

    @pl.when(is_r)
    def _():
        arrived(other.at[pl.ds(0, quarter)], qsend.at[0])
        arrived(other.at[pl.ds(0, direct)], qsend.at[1])
        arrived(other.at[pl.ds(0, (QUARTER + (QUARTER + 1) // 2) * ROWS)], qsend.at[2])
        arrived(other.at[pl.ds(0, 4 * quarter)], qsend.at[4])
        arrived(other.at[pl.ds(0, direct)], qsend.at[5])

    @pl.when(is_s)
    def _():
        arrived(other.at[pl.ds(0, (QUARTER + QUARTER // 2) * ROWS)], qsend.at[3])


def copy_kernel(pick, *refs):
    *sources, out = refs
    choice = pick[pl.program_id(0)]
    for k, ref in enumerate(sources):
        @pl.when(choice == k)
        def _():
            out[...] = ref[...].reshape(out.shape)

    @pl.when(choice == len(sources))
    def _():
        out[...] = jnp.zeros_like(out)


def pick_layers(picks, where, to, sources, shape, rows, base=None):
    blocks = shape[-2] // rows
    count = picks.shape[0]
    table = jnp.concatenate([picks, where, to]).astype(jnp.int32)

    def spec(k, source):
        lead = (1,) * (len(source.shape) - 2)

        def index(n, i, t):
            on = t[n] == k
            return (jnp.where(on, t[count + n], 0),) + (0,) * (len(lead) - 1) + (jnp.where(on, i, 0), 0)

        return pl.BlockSpec(lead + (rows, shape[-1]), index)

    lead = (1,) * (len(shape) - 2)
    extra = [] if base is None else [base]
    body = copy_kernel if base is None else lambda pick, kept, *refs: copy_kernel(pick, *refs)
    return pl.pallas_call(
        body,
        grid_spec=pltpu.PrefetchScalarGridSpec(
            num_scalar_prefetch=1,
            grid=(count, blocks),
            in_specs=[ANY] * len(extra) + [spec(k, source) for k, source in enumerate(sources)],
            out_specs=pl.BlockSpec(
                lead + (rows, shape[-1]), lambda n, i, t: (t[2 * count + n],) + (0,) * (len(lead) - 1) + (i, 0)),
        ),
        out_shape=jax.ShapeDtypeStruct(shape, BF16),
        input_output_aliases={} if base is None else {1: 0},
        cost_estimate=pl.CostEstimate(flops=0, bytes_accessed=4 * count * shape[-2] * shape[-1], transcendentals=0),
    )(table, *extra, *sources)


def permute_pairs(swap):
    pairs = [(z * 8 + e, 2 * e + (1 - z if swap else z)) for z in range(2) for e in range(8)]
    return [(a, b) for a, b in pairs if a != b]


def solution(mesh):
    flat_axes = ('stage', 'expert')
    DMA = pltpu.SemaphoreType.DMA
    side = pltpu.CompilerParams(has_side_effects=True)
    u13 = jax.ShapeDtypeStruct((4, 1, 2048, 1024), BF16)
    u2 = jax.ShapeDtypeStruct((4, 1, 512, 2048), BF16)

    def spread(unit, layer):
        out_shape = (u13, u2, jax.ShapeDtypeStruct((2048, 2048), BF16))
        buffers = []
        if layer == 0:
            out_shape += (jax.ShapeDtypeStruct((2, 2048, 1024), BF16),) + (jax.ShapeDtypeStruct((2048, 1024), BF16),) * 2
            buffers = [DMA((3, 3)), pltpu.VMEM((2, 2, 2048, 1024), BF16)]

        def call(*args):
            return pl.pallas_call(
                lambda *refs: spread_kernel(unit, layer, *refs),
                out_shape=out_shape,
                in_specs=[ANY] * 4,
                out_specs=(ANY,) * len(out_shape),
                scratch_shapes=[DMA((6, CHUNKS)), DMA((6, 4)), DMA((4, QUARTER)), DMA((DIRECT,)), DMA((6,))] + buffers,
                compiler_params=side,
                cost_estimate=pl.CostEstimate(flops=0, bytes_accessed=300 << 20, transcendentals=0),
            )(*args)

        return call

    def local_move(w_gate, w_up, w_down, dense, hot_ids, spare_map):
        stage = lax.axis_index('stage').astype(jnp.int32)
        core = (lax.axis_index('expert') % 2).astype(jnp.int32)
        layers = jnp.arange(4, dtype=jnp.int32)

        def permute(value, swap):
            return lax.ppermute(value, flat_axes, permute_pairs(swap))

        def slice2(piece):
            return pl.pallas_call(
                lambda t, ref, out: copy_kernel(t, ref, out),
                grid_spec=pltpu.PrefetchScalarGridSpec(
                    num_scalar_prefetch=1,
                    grid=(2, 2),
                    in_specs=[pl.BlockSpec((1, 1, 256, 2048), lambda l, i, t: (l, 0, 2 * t[2] + i, 0))],
                    out_specs=pl.BlockSpec((1, 256, 2048), lambda l, i, t: (l, i, 0)),
                ),
                out_shape=jax.ShapeDtypeStruct((2, 512, 2048), BF16),
            )(jnp.stack([0 * piece, 0 * piece, piece]), w_down)

        own2 = slice2(stage)
        own2, later = lax.optimization_barrier((own2, stage))
        a2 = permute(own2, 0)
        far2 = slice2(1 - later)

        def spread_all(unit, h):
            branches = [spread(root, h) for root in range(16)]
            return lax.switch(unit, branches, w_gate, w_up, w_down, dense)

        far2, first = lax.optimization_barrier((far2, hot_ids[0]))
        b2 = permute(far2, 1)
        h13, h2, o0, own13, far_a, far_b = spread_all(first, 0)
        second, o0 = lax.optimization_barrier((hot_ids[1], o0))
        a13 = permute(own13, 0)
        g13, g2, o1 = spread_all(second, 1)
        far_a, far_b, o1 = lax.optimization_barrier((far_a, far_b, o1))
        far_a = permute(far_a, 1)
        far_b = permute(far_b, 1)

        dense_all = pick_layers(
            jnp.where(layers // 2 == stage, 0, 1 + layers % 2), jnp.where(layers // 2 == stage, layers % 2, 0), layers,
            (dense, o0.reshape(1, 2048, 2048), o1.reshape(1, 2048, 2048)), (4, 2048, 2048), 1024)
        want = jnp.where(spare_map[0] < 0, 2, spare_map[0]) + 0 * layers
        spare13 = pick_layers(want, layers, layers, (h13, g13), u13.shape, 2048)
        spare2 = pick_layers(want, layers, layers, (h2, g2), u2.shape, 512)

        flat = stage * 8 + lax.axis_index('expert').astype(jnp.int32)
        keeps = jnp.where((flat == 0) | (flat == 15), 1, 0)
        pair, zero = layers[:2], 0 * layers
        w2 = pick_layers(jnp.where(layers // 2 == core, keeps, 2), layers % 2, layers, (a2, own2, b2), u2.shape, 512)
        w13 = pick_layers(keeps + 0 * pair, pair, 2 * core + pair, (a13, own13), u13.shape, 2048)
        for n, far in enumerate((far_a, far_b)):
            w13 = pick_layers(zero[:1], zero[:1], (2 - 2 * core + n).reshape(1), (far.reshape(1, 2048, 1024),),
                              u13.shape, 1024, w13)
        return w13, w2, dense_all, spare13, spare2

    expert_spec = P('stage', 'expert', None, None)
    unit_spec = P(None, flat_axes, None, None)

    return jax.shard_map(
        local_move,
        mesh=mesh,
        in_specs=(expert_spec, expert_spec, expert_spec, P('stage', None, None), P(None), P(flat_axes)),
        out_specs=(unit_spec, unit_spec, P(None, None, None), unit_spec, unit_spec),
        check_vma=False,
    )
```
